128 devices in a mesh: row: 8 (over x, core), col: 16 (over z, y).
Axes of the slice: x: 4, y: 4, z: 4, core: 2. Of those that a mesh axis runs over, the one named last changes fastest.
Arguments:
- tokens: bfloat16 [1024, 7168], P(('row', 'col')), may hold values from -6 to 6
- router_logits: float32 [1024, 16], P(('row', 'col')), may hold values from -18 to 318
- expert_ids: int32 [1024, 8], P(('row', 'col')), may hold values from 0 to 15, all different within a row; in each aligned block of 8 rows (0 to 7, 8 to 15, ...) at most 8 rows name the same one
- w_gate: bfloat16 [16, 7168, 2048], P('row', None, 'col'), may hold values from -0.3307189 to 0.3307189
- w_up: bfloat16 [16, 7168, 2048], P('row', None, 'col'), may hold values from -0.3307189 to 0.3307189
- w_down: bfloat16 [16, 2048, 7168], P('row', 'col'), may hold values from -0.61871843 to 0.61871843
Outputs:
- merged: bfloat16 [1024, 7168], P(('row', 'col'))
The draws below stay inside these ranges and needn't reach their ends.
Inputs may be any that keep to these rules, and one draw needn't show every extreme that they name: `expert_ids`: each row names 8 different experts. Among the 8 tokens of one device no expert is named more than 8 times, and in every draw some device names some expert exactly 8 times.
All inputs are finite; a program needn't handle non-finite values.
Results may differ from the reference program's by a relative error of at most 0.015.
Values may be sent and summed in bfloat16 or wider, within the bound.
No kernel may reach another device: no remote copies, remote signals or barrier semaphores. Data moves between devices by JAX's collectives and lax.ppermute only.
A program may use at most 128 MiB of HBM per device.

```python
import math
import jax
import jax.numpy as jnp
import numpy as np
from jax import lax

D = 7168
FF = 2048
TOP = 8
EXP_ROW = 2
TOK_DEV = 8
EXPERTS = 16
TOKENS = 1024
CAP = 8
N_ROW = 8
N_COL = 16


def expert_levels(key):
    groups = EXPERTS // EXP_ROW
    count = max(1, groups // 4)
    order = jax.random.permutation(jax.random.fold_in(key, 5), groups)
    group_flags = (order < count).astype(jnp.float32)
    return jnp.repeat(group_flags, EXP_ROW)


def scaled_weight(key, salt, shape, fan_in):
    flags = expert_levels(key)
    factor = 1.0 + 7.0 * flags
    values = jnp.clip(jax.random.normal(jax.random.fold_in(key, salt), shape, jnp.float32), -3.5, 3.5)
    values = values * factor[:, None, None] * fan_in ** (-0.5)
    return values.astype(jnp.bfloat16)


def draw_router_logits(key, part):
    first = jax.random.fold_in(key, 11)
    flags = expert_levels(key)
    noise = jax.random.normal(first, (TOKENS, EXPERTS), jnp.float32)
    base = jnp.where(flags[None, :] > 0.5, -4.5 + 0.5 * noise, 1.5 * noise)
    base = jnp.clip(base, -18.0, 18.0)
    return base


def draw_w_gate(key, part):
    return scaled_weight(key, 21, (EXPERTS, D, FF), D)


def draw_w_up(key, part):
    return scaled_weight(key, 22, (EXPERTS, D, FF), D)


def draw_w_down(key, part):
    return scaled_weight(key, 23, (EXPERTS, FF, D), FF)


def levels(stream_key, dims, cuts, smallest, high):
    def one(dim, blocks):
        draws = jax.random.uniform(jax.random.fold_in(jax.random.fold_in(stream_key, 6), dim), (blocks,), jnp.float32, smallest / len(cuts), high / len(cuts))
        return jnp.repeat(jnp.exp(draws), dims[dim] // blocks).reshape((-1,) + (1,) * (len(dims) - dim - 1))

    level = one(*cuts[0])
    for cut in cuts[1:]:
        level = level * one(*cut)
    return level


def deal_out(stream_key, own, number, rows, amount, top, most, lean):
    sequence = jax.random.permutation(stream_key, amount)
    packed, common = portions_of(amount, rows * top, most, lean, True), portions_of(amount, rows * top, most, lean, False)
    places = jnp.arange(amount)

    def named(sizes, offset_by):
        used = int((sizes > 0).sum())
        fixed = max(1, used // 4)
        moved = fixed + (places - fixed + offset_by * (used - fixed)) % max(1, amount - fixed)
        return jnp.zeros((amount,), jnp.int32).at[sequence[jnp.where(places < fixed, places, moved)]].set(jnp.asarray(sizes, jnp.int32))

    sizes = jnp.where(number % 4 == 0, named(packed, number // 4), named(common, number - number // 4 - 1))
    mixed = jax.random.permutation(jax.random.fold_in(own, 3), amount)
    giver, receiver = mixed[0:amount // 2 * 2:2], mixed[1:amount // 2 * 2:2]
    slack = jnp.minimum(sizes[giver] - 1, most - sizes[receiver]) // 2
    slack = jnp.where((giver == sequence[0]) | (receiver == sequence[0]) | (sizes[receiver] == 0), 0, jnp.maximum(slack, 0))
    moved = jax.random.randint(jax.random.fold_in(own, 4), (amount // 2,), 0, 1 << 20) % (slack + 1)
    sizes = sizes.at[giver].add(-moved).at[receiver].add(moved)
    members = jnp.searchsorted(jnp.cumsum(sizes), jnp.arange(rows * top), side="right").astype(jnp.int32)
    listing = members.reshape(top, rows).T
    listing = listing[jax.random.permutation(jax.random.fold_in(own, 1), rows)]
    offset_by = jax.random.randint(jax.random.fold_in(own, 2), (rows, 1), 0, top)
    return jnp.take_along_axis(listing, (jnp.arange(top)[None, :] + offset_by) % top, axis=1)


def portions_of(number_of, total, bound, slope, full):
    portions = [(1 << 20) // math.isqrt(grade ** slope) + 1 for grade in range(1, number_of + 1)]
    largest = bound if full else min(bound, max(-(-total // number_of), total * portions[0] // sum(portions)))
    least = 1 if total - largest >= number_of - 1 else 0
    counts, surplus = [largest] + [least] * (number_of - 1), total - largest - least * (number_of - 1)
    while surplus > 0:
        free = [i for i in range(1, number_of) if counts[i] < largest] or [i for i in range(1, number_of) if counts[i] < bound]
        pool, left = sum([portions[i] for i in free]), surplus
        for i in free:
            extra = min(bound - counts[i], max(1, left * portions[i] // pool), surplus)
            counts[i] = counts[i] + extra
            surplus = surplus - extra
    return np.array(counts)


def scatter_about(rng, dims, deviation, bound, shards=(), kind=jnp.bfloat16):
    array = deviation * jax.random.normal(rng, dims, jnp.float32)
    if shards:
        array = array * levels(rng, dims, shards, -0.22, 0.18)
    return jnp.clip(array, -bound, bound).astype(kind)


def setup_inputs(seed: int = 0) -> dict:
    keys = jax.random.split(jax.random.key(seed), 7)
    tokens = scatter_about(keys[0], (TOKENS, D), 1.0, 6.0, ((0, 128),))
    router_logits = draw_router_logits(jax.random.fold_in(keys[6], 71), 0)
    expert_ids_keys = jax.random.split(jax.random.fold_in(keys[2], 1), TOKENS // TOK_DEV)
    expert_ids_turns = jax.random.permutation(jax.random.fold_in(keys[2], 3), TOKENS // TOK_DEV)
    expert_ids = jax.vmap(lambda own, number: deal_out(jax.random.fold_in(keys[2], 2), own, number, TOK_DEV, EXPERTS, TOP, CAP, 2))(expert_ids_keys, expert_ids_turns).reshape((TOKENS, TOP))
    w_gate = draw_w_gate(jax.random.fold_in(keys[6], 71), 0)
    w_up = draw_w_up(jax.random.fold_in(keys[6], 71), 0)
    w_down = draw_w_down(jax.random.fold_in(keys[6], 71), 0)
    return dict(tokens=tokens, router_logits=router_logits, expert_ids=expert_ids, w_gate=w_gate, w_up=w_up, w_down=w_down)


def reference(tokens, router_logits, expert_ids, w_gate, w_up, w_down):
    picked = jnp.take_along_axis(router_logits, expert_ids, axis=1)
    probs = lax.optimization_barrier(jax.nn.softmax(picked, axis=-1).astype(jnp.bfloat16)).astype(jnp.float32)
    marks = expert_ids[:, :, None] == jnp.arange(EXPERTS, dtype=jnp.int32)[None, None, :]
    table = jnp.sum(probs[:, :, None] * marks.astype(jnp.float32), axis=1)
    picks = jnp.any(marks, axis=1).astype(jnp.int32)
    slice_width = FF // N_COL
    per_group = EXPERTS // N_ROW
    limit = min(TOKENS, CAP * N_ROW * N_COL)

    def group_sum(total, group):
        terms = jnp.zeros((N_COL, TOKENS, D), jnp.float32)
        for inner in range(per_group):
            expert = group * per_group + inner
            flags = lax.dynamic_index_in_dim(picks, expert, 1, keepdims=False)
            order = jnp.argsort(1 - flags, stable=True)[:limit].astype(jnp.int32)
            chosen_rows = tokens[order]
            gate = jnp.dot(chosen_rows, w_gate[expert], preferred_element_type=jnp.float32)
            up = jnp.dot(chosen_rows, w_up[expert], preferred_element_type=jnp.float32)
            hidden = (jax.nn.silu(gate) * up).astype(jnp.bfloat16)
            sliced = hidden.astype(jnp.float32).reshape(limit, N_COL, slice_width)
            down = w_down[expert].astype(jnp.float32).reshape(N_COL, slice_width, D)
            outputs = jnp.einsum("tcf,cfd->ctd", sliced, down, precision=lax.Precision.HIGHEST)
            weight = lax.dynamic_index_in_dim(table, expert, 1, keepdims=False)[order]
            terms = terms.at[:, order].add(outputs * weight[None, :, None])
        rounded = lax.optimization_barrier(terms.astype(jnp.bfloat16)).astype(jnp.float32)
        group_out = lax.optimization_barrier(jnp.sum(rounded, axis=0).astype(jnp.bfloat16)).astype(jnp.float32)
        return total + group_out, None

    total, _ = lax.scan(group_sum, jnp.zeros((TOKENS, D), jnp.float32), jnp.arange(N_ROW, dtype=jnp.int32))
    return total.astype(jnp.bfloat16)
```

```python
import jax
import jax.numpy as jnp
from jax import lax
from jax.sharding import PartitionSpec as P

AXES = ("row", "col")
ORDER = (("x", "y", "z"), ("y", "z", "x"))


def place(row, col):
    return {"x": row // 2, "core": row % 2, "z": col // 4, "y": col % 4}


def index(at):
    return (at["x"] * 2 + at["core"]) * 16 + at["z"] * 4 + at["y"]


def pairs(phase, shift):
    moves = []
    for row in range(8):
        for col in range(16):
            at = place(row, col)
            to = dict(at)
            axis = ORDER[at["core"]][phase]
            to[axis] = (to[axis] + shift) % 4
            moves.append((index(at), index(to)))
    return moves


def fetch(value, phase, shift):
    return lax.ppermute(value, AXES, pairs(phase, -shift))


def swap(value):
    return lax.ppermute(value, AXES, [(i, i ^ 16) for i in range(128)])


def local(tokens, router_logits, expert_ids, w_gate, w_up, w_down):
    experts = router_logits.shape[1]
    per_group = w_gate.shape[0]
    width = tokens.shape[1]
    marks = expert_ids[:, :, None] == jnp.arange(experts, dtype=jnp.int32)[None, None, :]
    chosen = jnp.any(marks, axis=1)
    table = jax.nn.softmax(jnp.where(chosen, router_logits, -jnp.inf), axis=-1).astype(jnp.bfloat16)
    block = jnp.concatenate([tokens, jnp.pad(table, ((0, 0), (0, 128 - experts)))], axis=1)

    w_in = jnp.concatenate([w_gate[0], w_gate[1], w_up[0], w_up[1]], axis=1)
    w_out = w_down.reshape(-1, width)
    first = lax.axis_index("row") * per_group

    for phase in range(2):
        block = jnp.concatenate([block] + [fetch(block, phase, k) for k in (1, 2, 3)], axis=0)
    own = [block] + [fetch(block, 2, k) for k in (1, 2, 3)]
    other = [swap(piece) for piece in own]

    def experts_of(piece):
        weight = lax.dynamic_slice_in_dim(piece[:, width:], first, per_group, 1).astype(jnp.float32)
        both = jnp.dot(piece[:, :width], w_in, preferred_element_type=jnp.float32)
        half = both.shape[1] // 2
        hidden = jax.nn.silu(both[:, :half]) * both[:, half:]
        hidden = hidden.reshape(hidden.shape[0], per_group, -1) * weight[:, :, None]
        hidden = hidden.astype(jnp.bfloat16).reshape(hidden.shape[0], -1)
        return jnp.dot(hidden, w_out, preferred_element_type=jnp.float32)

    sums = []
    for k in range(4):
        back = swap(experts_of(other[k]).astype(jnp.bfloat16))
        sums.append((experts_of(own[k]) + back.astype(jnp.float32)).astype(jnp.bfloat16))
    for phase in (2, 1, 0):
        got = [fetch(sums[k], phase, -k) for k in (1, 2, 3)]
        total = sums[0].astype(jnp.float32)
        for piece in got:
            total = total + piece.astype(jnp.float32)
        total = total.astype(jnp.bfloat16)
        if phase:
            rows = total.shape[0] // 4
            sums = [total[k * rows : (k + 1) * rows] for k in range(4)]
    return total


def solution(mesh):
    in_specs = (
        P(("row", "col"), None),
        P(("row", "col"), None),
        P(("row", "col"), None),
        P("row", None, "col"),
        P("row", None, "col"),
        P("row", "col", None),
    )
    out_specs = P(("row", "col"), None)
    return jax.shard_map(local, mesh=mesh, in_specs=in_specs, out_specs=out_specs, check_vma=False)
```

```python
import jax
import jax.numpy as jnp
from jax import lax
from jax.experimental import pallas as pl
from jax.experimental.pallas import tpu as pltpu
from jax.sharding import PartitionSpec as P


AXES = ("row", "col")
ORDER = (("x", "y", "z"), ("y", "z", "x"))
VMEM = pl.BlockSpec(memory_space=pltpu.VMEM)


def place(row, col):
    return {"x": row // 2, "core": row % 2, "z": col // 4, "y": col % 4}


def index(at):
    return (at["x"] * 2 + at["core"]) * 16 + at["z"] * 4 + at["y"]


def pairs(phase, shift):
    moves = []
    for row in range(8):
        for col in range(16):
            at = place(row, col)
            to = dict(at)
            axis = ORDER[at["core"]][phase]
            to[axis] = (to[axis] + shift) % 4
            moves.append((index(at), index(to)))
    return moves


def send(value, phase, shift):
    return lax.ppermute(value, AXES, pairs(phase, shift))


def swap(value):
    return lax.ppermute(value, AXES, [(i, i ^ 16) for i in range(128)])


def route_kernel(tokens, logits, ids, block):
    width = tokens.shape[1]
    experts = logits.shape[1]
    names = lax.broadcasted_iota(jnp.int32, logits.shape, 1)
    chosen = ids[:, 0:1] == names
    for k in range(1, ids.shape[1]):
        chosen = chosen | (ids[:, k : k + 1] == names)
    scores = jnp.where(chosen, logits[...], -jnp.inf)
    scores = jnp.exp(scores - jnp.max(scores, axis=1, keepdims=True))
    probs = scores / jnp.sum(scores, axis=1, keepdims=True)
    block[:, :width] = tokens[...]
    block[:, width:] = jnp.zeros((tokens.shape[0], 128), block.dtype)
    block[:, width : width + experts] = probs.astype(block.dtype)


def expert_kernel(*refs):
    rows_a, rows_b, spread, w_in, w_out = refs[:5]
    back = refs[5:-3]
    out_a, out_b, rows = refs[-3:]
    half, width = out_a.shape
    rows[:half, :] = rows_a[...]
    rows[half:, :] = rows_b[...]
    weight = jnp.dot(rows[:, width:], spread[...], preferred_element_type=jnp.float32)
    both = jnp.dot(rows[:, :width], w_in[...], preferred_element_type=jnp.float32)
    units = both.shape[1] // 2
    gate = both[:, :units]
    hidden = gate / (1.0 + jnp.exp(-gate)) * both[:, units:] * weight
    hidden = hidden.astype(rows.dtype)
    step = width // 7
    for j in range(7):
        at = slice(j * step, (j + 1) * step)
        part = jnp.dot(hidden, w_out[:, at], preferred_element_type=jnp.float32)
        part_a, part_b = part[:half], part[half:]
        if back:
            part_a = part_a + back[0][:, at].astype(jnp.float32)
            part_b = part_b + back[1][:, at].astype(jnp.float32)
        out_a[:, at] = part_a.astype(out_a.dtype)
        out_b[:, at] = part_b.astype(out_b.dtype)


def experts_of(rows, weights, back=()):
    half, packed = rows[0].shape
    width = weights[2].shape[1]
    shape = jax.ShapeDtypeStruct((half, width), rows[0].dtype)
    return pl.pallas_call(
        expert_kernel,
        out_shape=(shape, shape),
        in_specs=[VMEM] * (5 + len(back)),
        out_specs=(VMEM, VMEM),
        scratch_shapes=[pltpu.VMEM((2 * half, packed), rows[0].dtype)],
        compiler_params=pltpu.CompilerParams(vmem_limit_bytes=24 << 20),
        cost_estimate=pl.CostEstimate(
            flops=2 * 2 * half * width * 768, bytes_accessed=half * width * 12, transcendentals=2 * half * 256
        ),
        name="experts",
    )(*rows, *weights, *back)


def add_kernel(count, *refs):
    total = refs[0][...].astype(jnp.float32)
    for piece in refs[1:count]:
        total = total + piece[...].astype(jnp.float32)
    total = total.astype(refs[0].dtype)
    outs = refs[count:]
    rows = total.shape[0] // len(outs)
    for k, out in enumerate(outs):
        out[...] = total[k * rows : (k + 1) * rows]


def add(pieces, parts):
    rows, width = pieces[0].shape
    shape = jax.ShapeDtypeStruct((rows // parts, width), pieces[0].dtype)

    def kernel(*refs):
        add_kernel(len(pieces), *refs)

    return pl.pallas_call(
        kernel,
        out_shape=(shape,) * parts,
        in_specs=[VMEM] * len(pieces),
        out_specs=(VMEM,) * parts,
        compiler_params=pltpu.CompilerParams(vmem_limit_bytes=12 << 20),
        name="add",
    )(*pieces)


def local(tokens, router_logits, expert_ids, w_gate, w_up, w_down):
    per_group = w_gate.shape[0]
    units = w_gate.shape[2]
    count, width = tokens.shape
    block = pl.pallas_call(
        route_kernel,
        out_shape=jax.ShapeDtypeStruct((count, width + 128), tokens.dtype),
        compiler_params=pltpu.CompilerParams(vmem_limit_bytes=4 << 20),
        name="route",
    )(tokens, router_logits, expert_ids)

    w_in = jnp.concatenate([w_gate[0], w_gate[1], w_up[0], w_up[1]], axis=1)
    names = lax.axis_index("row") * per_group + jnp.arange(per_group * units) // units
    spread = (jnp.arange(128)[:, None] == names[None, :]).astype(jnp.bfloat16)
    weights = (spread, w_in, w_down.reshape(-1, width))

    got = [send(block, 0, -k) for k in (1, 3, 2)]
    block = lax.optimization_barrier(jnp.concatenate([block, got[0], got[1], got[2]], axis=0))
    got = [send(block, 1, -k) for k in (1, 3, 2)]
    a0 = lax.optimization_barrier(jnp.concatenate([block, got[0]], axis=0))
    b0 = lax.optimization_barrier(jnp.concatenate([got[1], got[2]], axis=0))

    am, bp = send(a0, 2, 1), send(b0, 2, -1)
    bm, ap = send(b0, 2, 1), send(a0, 2, -1)
    oa, ob = send(am, 2, 1), send(bp, 2, -1)

    def answer(a, b):
        there = (swap(a), swap(b))
        there = experts_of(there, weights)
        back = (swap(there[0]), swap(there[1]))
        return experts_of((a, b), weights, back)

    sa0, sb0 = answer(a0, b0)
    sam, sbp = answer(am, bp)
    sap, sbm = answer(ap, bm)
    soa, sob = answer(oa, ob)

    direct_b = send(sbp, 2, 1)
    direct_a = send(sam, 2, -1)
    over_a = send(soa, 2, 1)
    over_b = send(sob, 2, -1)
    relay_a = send(add((sap, over_a), 1)[0], 2, 1)
    relay_b = send(add((sbm, over_b), 1)[0], 2, -1)
    sums = add((sa0, direct_a, relay_a), 2) + add((sb0, direct_b, relay_b), 2)
    got = [send(sums[j], 1, k) for j, k in ((1, 1), (2, 3), (3, 2))]
    sums = add((sums[0], *got), 4)
    got = [send(sums[j], 0, k) for j, k in ((1, 1), (2, 3), (3, 2))]
    return add((sums[0], *got), 1)[0]


def solution(mesh):
    in_specs = (
        P(("row", "col"), None),
        P(("row", "col"), None),
        P(("row", "col"), None),
        P("row", None, "col"),
        P("row", None, "col"),
        P("row", "col", None),
    )
    out_specs = P(("row", "col"), None)
    return jax.shard_map(local, mesh=mesh, in_specs=in_specs, out_specs=out_specs, check_vma=False)
```

```python
import functools

import jax
import jax.numpy as jnp
from jax import lax
from jax.experimental import pallas as pl
from jax.experimental.pallas import tpu as pltpu
from jax.sharding import PartitionSpec as P


AXES = ("row", "col")
ORDER = (("x", "y", "z"), ("y", "z", "x"))
HBM = pl.BlockSpec(memory_space=pltpu.HBM)
VMEM = pl.BlockSpec(memory_space=pltpu.VMEM)


def place(row, col):
    return {"x": row // 2, "core": row % 2, "z": col // 4, "y": col % 4}


def index(at):
    return (at["x"] * 2 + at["core"]) * 16 + at["z"] * 4 + at["y"]


def pairs(phase, shift):
    moves = []
    for row in range(8):
        for col in range(16):
            at = place(row, col)
            to = dict(at)
            axis = ORDER[at["core"]][phase]
            to[axis] = (to[axis] + shift) % 4
            moves.append((index(at), index(to)))
    return moves


def send(value, phase, shift):
    return lax.ppermute(value, AXES, pairs(phase, shift))


def swap(value):
    return lax.ppermute(value, AXES, [(i, i ^ 16) for i in range(128)])


def route_kernel(tokens, routing, block):
    width = tokens.shape[1]
    logits = routing[:, :16]
    names = lax.broadcasted_iota(jnp.int32, logits.shape, 1).astype(jnp.float32)
    chosen = routing[:, 16:17] == names
    for k in range(17, routing.shape[1]):
        chosen = chosen | (routing[:, k : k + 1] == names)
    scores = jnp.where(chosen, logits, -jnp.inf)
    scores = jnp.exp(scores - jnp.max(scores, axis=1, keepdims=True))
    probs = scores / jnp.sum(scores, axis=1, keepdims=True)
    block[:, :width] = tokens[...]
    block[:, width:] = jnp.zeros((block.shape[0], 128), block.dtype)
    block[:, width : width + 16] = probs.astype(block.dtype)


def join_kernel(places, *refs):
    out = refs[-1]
    for (row, col), ref in zip(places, refs[:-1]):
        out[row : row + ref.shape[0], col : col + ref.shape[1]] = ref[...]


def join(rows, cols, *pieces):
    arrays = [piece for piece, _, _ in pieces]
    places = tuple((row, col) for _, row, col in pieces)
    return pl.pallas_call(
        functools.partial(join_kernel, places),
        out_shape=jax.ShapeDtypeStruct((rows, cols), arrays[0].dtype),
        in_specs=[VMEM] * len(arrays),
        out_specs=VMEM,
        compiler_params=pltpu.CompilerParams(vmem_limit_bytes=6 << 20),
        name="join",
    )(*arrays)


def pack_kernel(gate, up, packed, sems):
    per_group, _, units = gate.shape
    copies = []
    for j, weight in enumerate((gate, up)):
        for e in range(per_group):
            k = j * per_group + e
            to = packed.at[:, pl.ds(k * units, units)]
            copies.append(pltpu.make_async_copy(weight.at[e], to, sems.at[k]))
    for copy in copies:
        copy.start()
    for copy in copies:
        copy.wait()


def expert_kernel(piece_a, piece_b, spread, in_own, in_other, down_own, down_other, out_a, out_b, rows):
    half, width = out_a.shape
    rows[:half, :] = piece_a[...]
    rows[half:, :] = piece_b[...]
    weight = jnp.dot(rows[:, width:], spread[...], preferred_element_type=jnp.float32)
    hidden = []
    for k, w_in in enumerate((in_own, in_other)):
        both = jnp.dot(rows[:, :width], w_in[...], preferred_element_type=jnp.float32)
        units = both.shape[1] // 2
        gate = both[:, :units]
        value = gate / (1.0 + jnp.exp(-gate)) * both[:, units:] * weight[:, k * units : (k + 1) * units]
        hidden.append(value.astype(rows.dtype))
    step = width // 7
    for j in range(7):
        cols = slice(j * step, (j + 1) * step)
        part = jnp.dot(hidden[0], down_own[:, cols], preferred_element_type=jnp.float32)
        part = part + jnp.dot(hidden[1], down_other[:, cols], preferred_element_type=jnp.float32)
        part = part.astype(out_a.dtype)
        out_a[:, cols] = part[:half]
        out_b[:, cols] = part[half:]


def experts_of(piece_a, piece_b, weights):
    half, packed = piece_a.shape
    width = packed - 128
    kind = piece_a.dtype
    shape = jax.ShapeDtypeStruct((half, width), kind)
    return pl.pallas_call(
        expert_kernel,
        out_shape=(shape, shape),
        in_specs=[VMEM] * 7,
        out_specs=(VMEM,) * 2,
        scratch_shapes=[pltpu.VMEM((2 * half, packed), kind)],
        compiler_params=pltpu.CompilerParams(vmem_limit_bytes=12 << 20),
        cost_estimate=pl.CostEstimate(
            flops=4 * half * width * 1536, bytes_accessed=half * width * 8, transcendentals=half * 1024
        ),
        name="experts",
    )(piece_a, piece_b, *weights)


def pack(gate, up):
    per_group, width, units = gate.shape
    return pl.pallas_call(
        pack_kernel,
        out_shape=jax.ShapeDtypeStruct((width, 2 * per_group * units), gate.dtype),
        in_specs=[HBM] * 2,
        out_specs=VMEM,
        scratch_shapes=[pltpu.SemaphoreType.DMA((2 * per_group,))],
        compiler_params=pltpu.CompilerParams(vmem_limit_bytes=2 << 20),
        name="pack",
    )(gate, up)


def add_kernel(starts, *refs):
    out = refs[-1]
    total = None
    for start, ref in zip(starts, refs[:-1]):
        piece = ref[start : start + out.shape[0], :].astype(jnp.float32)
        total = piece if total is None else total + piece
    out[...] = total.astype(out.dtype)


def add(rows, *pieces):
    arrays = [piece for piece, _ in pieces]
    starts = tuple(start for _, start in pieces)
    return pl.pallas_call(
        functools.partial(add_kernel, starts),
        out_shape=jax.ShapeDtypeStruct((rows, arrays[0].shape[1]), arrays[0].dtype),
        in_specs=[VMEM] * len(arrays),
        out_specs=VMEM,
        compiler_params=pltpu.CompilerParams(vmem_limit_bytes=6 << 20),
        name="add",
    )(*arrays)


def local(tokens, router_logits, expert_ids, w_gate, w_up, w_down):
    per_group, _, units = w_gate.shape
    count, width = tokens.shape
    packed = width + 128
    near = (1, 3, 2)
    routing = jnp.concatenate([router_logits, expert_ids.astype(jnp.float32)], axis=1)
    block = pl.pallas_call(
        route_kernel,
        out_shape=jax.ShapeDtypeStruct((count, packed), tokens.dtype),
        in_specs=[VMEM] * 2,
        out_specs=VMEM,
        compiler_params=pltpu.CompilerParams(vmem_limit_bytes=2 << 20),
        name="route",
    )(tokens, routing)
    got = [send(block, 0, -k) for k in near]
    gate_other, up_other, down_other = swap(w_gate), swap(w_up), swap(w_down)
    block = join(4 * count, packed, *((piece, k * count, 0) for k, piece in enumerate([block, *got])))
    row = lax.axis_index("row")
    spot = jnp.arange(2 * per_group * units)
    names = jnp.where(spot < per_group * units, row, row ^ 1) * per_group + spot // units % per_group
    spread = (jnp.arange(128)[:, None] == names[None, :]).astype(jnp.bfloat16)

    got = [send(block, 1, -k) for k in near]
    weights = (
        spread, pack(w_gate, w_up), pack(gate_other, up_other), w_down.reshape(-1, width), down_other.reshape(-1, width)
    )
    a0 = join(8 * count, packed, (block, 0, 0), (got[0], 4 * count, 0))
    b0 = join(8 * count, packed, (got[1], 0, 0), (got[2], 4 * count, 0))
    am, bp = send(a0, 2, 1), send(b0, 2, -1)
    oa, ob = send(am, 2, 1), send(bp, 2, -1)
    bm, ap = send(b0, 2, 1), send(a0, 2, -1)

    half = 8 * count
    sa0, sb0 = experts_of(a0, b0, weights)
    sam, sbp = experts_of(am, bp, weights)
    soa, sob = experts_of(oa, ob, weights)
    sap, sbm = experts_of(ap, bm, weights)

    over_a = send(soa, 2, 1)
    over_b = send(sob, 2, -1)
    direct_b = send(sbp, 2, 1)
    direct_a = send(sam, 2, -1)
    relay_a = send(add(half, (sap, 0), (over_a, 0)), 2, 1)
    relay_b = send(add(half, (sbm, 0), (over_b, 0)), 2, -1)

    def group(at, *pieces):
        return add(4 * count, *((piece, at) for piece in pieces))

    got = [send(group(4 * count, sa0, direct_a, relay_a), 1, 1)]
    got.append(send(group(0, sb0, direct_b, relay_b), 1, 3))
    got.append(send(group(4 * count, sb0, direct_b, relay_b), 1, 2))
    pieces = (group(0, sa0, direct_a, relay_a), *got)
    sums = [add(count, *((piece, k * count) for piece in pieces)) for k in range(4)]
    got = [send(sums[j], 0, k) for j, k in ((1, 1), (2, 3), (3, 2))]
    return add(count, *((piece, 0) for piece in (sums[0], *got)))


def solution(mesh):
    in_specs = (
        P(("row", "col"), None),
        P(("row", "col"), None),
        P(("row", "col"), None),
        P("row", None, "col"),
        P("row", None, "col"),
        P("row", "col", None),
    )
    out_specs = P(("row", "col"), None)
    return jax.shard_map(local, mesh=mesh, in_specs=in_specs, out_specs=out_specs, check_vma=False)
```

```python
import functools

import jax
import jax.numpy as jnp
from jax import lax
from jax.experimental import pallas as pl
from jax.experimental.pallas import tpu as pltpu
from jax.sharding import PartitionSpec as P


AXES = ("row", "col")
ORDER = (("x", "y", "z"), ("y", "z", "x"))
HBM = pl.BlockSpec(memory_space=pltpu.HBM)
VMEM = pl.BlockSpec(memory_space=pltpu.VMEM)


def place(row, col):
    return {"x": row // 2, "core": row % 2, "z": col // 4, "y": col % 4}


def index(at):
    return (at["x"] * 2 + at["core"]) * 16 + at["z"] * 4 + at["y"]


def pairs(phase, shift):
    moves = []
    for row in range(8):
        for col in range(16):
            at = place(row, col)
            to = dict(at)
            axis = ORDER[at["core"]][phase]
            to[axis] = (to[axis] + shift) % 4
            moves.append((index(at), index(to)))
    return moves


def send(value, phase, shift):
    return lax.ppermute(value, AXES, pairs(phase, shift))


def swap(value):
    return lax.ppermute(value, AXES, [(i, i ^ 16) for i in range(128)])


def route_kernel(tokens, routing, block):
    width = tokens.shape[1]
    logits = routing[:, :16]
    names = lax.broadcasted_iota(jnp.int32, logits.shape, 1).astype(jnp.float32)
    chosen = routing[:, 16:17] == names
    for k in range(17, routing.shape[1]):
        chosen = chosen | (routing[:, k : k + 1] == names)
    scores = jnp.where(chosen, logits, -jnp.inf)
    scores = jnp.exp(scores - jnp.max(scores, axis=1, keepdims=True))
    probs = scores / jnp.sum(scores, axis=1, keepdims=True)
    block[:, :width] = tokens[...]
    block[:, width:] = jnp.zeros((block.shape[0], 128), block.dtype)
    block[:, width : width + 16] = probs.astype(block.dtype)


def join_kernel(places, *refs):
    out = refs[-1]
    for (row, col), ref in zip(places, refs[:-1]):
        out[row : row + ref.shape[0], col : col + ref.shape[1]] = ref[...]


def join(rows, cols, *pieces):
    arrays = [piece for piece, _, _ in pieces]
    places = tuple((row, col) for _, row, col in pieces)
    return pl.pallas_call(
        functools.partial(join_kernel, places),
        out_shape=jax.ShapeDtypeStruct((rows, cols), arrays[0].dtype),
        in_specs=[VMEM] * len(arrays),
        out_specs=VMEM,
        compiler_params=pltpu.CompilerParams(vmem_limit_bytes=6 << 20),
        name="join",
    )(*arrays)


def pack_kernel(gate, up, down, packed, kept, sems):
    per_group, _, units = gate.shape
    copies = [pltpu.make_async_copy(down, kept, sems.at[2 * per_group])]
    for j, weight in enumerate((gate, up)):
        for e in range(per_group):
            k = j * per_group + e
            to = packed.at[:, pl.ds(k * units, units)]
            copies.append(pltpu.make_async_copy(weight.at[e], to, sems.at[k]))
    for copy in copies:
        copy.start()
    for copy in copies:
        copy.wait()


def expert_kernel(piece_a, piece_b, spread, in_own, in_other, down_own, down_other, out_a, out_b, rows):
    half, width = out_a.shape
    rows[:half, :] = piece_a[...]
    rows[half:, :] = piece_b[...]
    weight = jnp.dot(rows[:, width:], spread[...], preferred_element_type=jnp.float32)
    hidden = []
    for k, w_in in enumerate((in_own, in_other)):
        both = jnp.dot(rows[:, :width], w_in[...], preferred_element_type=jnp.float32)
        units = both.shape[1] // 2
        gate = both[:, :units]
        value = gate / (1.0 + jnp.exp(-gate)) * both[:, units:] * weight[:, k * units : (k + 1) * units]
        hidden.append(value.astype(rows.dtype))
    step = width // 7
    for j in range(7):
        cols = slice(j * step, (j + 1) * step)
        part = jnp.dot(hidden[0], down_own[:, cols], preferred_element_type=jnp.float32)
        part = part + jnp.dot(hidden[1], down_other[:, cols], preferred_element_type=jnp.float32)
        part = part.astype(out_a.dtype)
        out_a[:, cols] = part[:half]
        out_b[:, cols] = part[half:]


def experts_of(piece_a, piece_b, weights):
    half, packed = piece_a.shape
    width = packed - 128
    kind = piece_a.dtype
    shape = jax.ShapeDtypeStruct((half, width), kind)
    return pl.pallas_call(
        expert_kernel,
        out_shape=(shape, shape),
        in_specs=[VMEM] * 7,
        out_specs=(VMEM,) * 2,
        scratch_shapes=[pltpu.VMEM((2 * half, packed), kind)],
        compiler_params=pltpu.CompilerParams(vmem_limit_bytes=12 << 20),
        cost_estimate=pl.CostEstimate(
            flops=4 * half * width * 1536, bytes_accessed=half * width * 8, transcendentals=half * 1024
        ),
        name="experts",
    )(piece_a, piece_b, *weights)


def pack(gate, up, down):
    per_group, width, units = gate.shape
    down = down.reshape(-1, width)
    return pl.pallas_call(
        pack_kernel,
        out_shape=(
            jax.ShapeDtypeStruct((width, 2 * per_group * units), gate.dtype),
            jax.ShapeDtypeStruct(down.shape, down.dtype),
        ),
        in_specs=[HBM] * 3,
        out_specs=(VMEM, VMEM),
        scratch_shapes=[pltpu.SemaphoreType.DMA((2 * per_group + 1,))],
        compiler_params=pltpu.CompilerParams(vmem_limit_bytes=2 << 20),
        name="pack",
    )(gate, up, down)


def add_kernel(starts, *refs):
    out = refs[-1]
    total = None
    for start, ref in zip(starts, refs[:-1]):
        piece = ref[start : start + out.shape[0], :].astype(jnp.float32)
        total = piece if total is None else total + piece
    out[...] = total.astype(out.dtype)


def add(rows, *pieces):
    arrays = [piece for piece, _ in pieces]
    starts = tuple(start for _, start in pieces)
    return pl.pallas_call(
        functools.partial(add_kernel, starts),
        out_shape=jax.ShapeDtypeStruct((rows, arrays[0].shape[1]), arrays[0].dtype),
        in_specs=[VMEM] * len(arrays),
        out_specs=VMEM,
        compiler_params=pltpu.CompilerParams(vmem_limit_bytes=6 << 20),
        name="add",
    )(*arrays)


def local(tokens, router_logits, expert_ids, w_gate, w_up, w_down):
    per_group, _, units = w_gate.shape
    count, width = tokens.shape
    packed = width + 128
    near = (1, 3, 2)
    routing = jnp.concatenate([router_logits, expert_ids.astype(jnp.float32)], axis=1)
    block = pl.pallas_call(
        route_kernel,
        out_shape=jax.ShapeDtypeStruct((count, packed), tokens.dtype),
        in_specs=[VMEM] * 2,
        out_specs=VMEM,
        compiler_params=pltpu.CompilerParams(vmem_limit_bytes=2 << 20),
        name="route",
    )(tokens, routing)
    got = [send(block, 0, -k) for k in near]
    gate_other, up_other, down_other = swap(w_gate), swap(w_up), swap(w_down)
    block = join(4 * count, packed, *((piece, k * count, 0) for k, piece in enumerate([block, *got])))
    row = lax.axis_index("row")
    spot = jnp.arange(2 * per_group * units)
    names = jnp.where(spot < per_group * units, row, row ^ 1) * per_group + spot // units % per_group
    spread = (jnp.arange(128)[:, None] == names[None, :]).astype(jnp.bfloat16)
    block, spread = lax.optimization_barrier((block, spread))

    got = [send(block, 1, -k) for k in near]
    in_own, down_own = pack(w_gate, w_up, w_down)
    in_other, down_other = pack(gate_other, up_other, down_other)
    weights = (spread, in_own, in_other, down_own, down_other)
    a0 = join(8 * count, packed, (block, 0, 0), (got[0], 4 * count, 0))
    b0 = join(8 * count, packed, (got[1], 0, 0), (got[2], 4 * count, 0))
    am, bp = send(a0, 2, 1), send(b0, 2, -1)
    oa, ob = send(am, 2, 1), send(bp, 2, -1)
    bm, ap = send(b0, 2, 1), send(a0, 2, -1)

    sa0, sb0 = experts_of(a0, b0, weights)
    sam, sbp = experts_of(am, bp, weights)
    soa, sob = experts_of(oa, ob, weights)
    sap, sbm = experts_of(ap, bm, weights)

    over_a = send(soa, 2, 1)
    over_b = send(sob, 2, -1)
    direct_b = send(sbp, 2, 1)
    direct_a = send(sam, 2, -1)
    part = 4 * count
    relay1 = send(add(part, (sap, part), (over_a, part)), 2, 1)
    relay2 = send(add(part, (sbm, part), (over_b, part)), 2, -1)
    relay0 = send(add(part, (sap, 0), (over_a, 0)), 2, 1)
    relay3 = send(add(part, (sbm, 0), (over_b, 0)), 2, -1)
    got = [send(add(part, (sa0, part), (direct_a, part), (relay1, 0)), 1, 1)]
    got.append(send(add(part, (sb0, part), (direct_b, part), (relay2, 0)), 1, 2))
    got.append(send(add(part, (sb0, 0), (direct_b, 0), (relay3, 0)), 1, 3))
    pieces = (add(part, (sa0, 0), (direct_a, 0), (relay0, 0)), *got)
    sums = [add(count, *((piece, k * count) for piece in pieces)) for k in range(4)]
    got = [send(sums[j], 0, k) for j, k in ((1, 1), (2, 3), (3, 2))]
    return add(count, *((piece, 0) for piece in (sums[0], *got)))


def solution(mesh):
    in_specs = (
        P(("row", "col"), None),
        P(("row", "col"), None),
        P(("row", "col"), None),
        P("row", None, "col"),
        P("row", None, "col"),
        P("row", "col", None),
    )
    out_specs = P(("row", "col"), None)
    return jax.shard_map(local, mesh=mesh, in_specs=in_specs, out_specs=out_specs, check_vma=False)
```

```python
import functools

import jax
import jax.numpy as jnp
from jax import lax
from jax.experimental import pallas as pl
from jax.experimental.pallas import tpu as pltpu
from jax.sharding import PartitionSpec as P


AXES = ("row", "col")
ORDER = (("y", "z", "x"), ("x", "y", "z"))
HBM = pl.BlockSpec(memory_space=pltpu.HBM)
VMEM = pl.BlockSpec(memory_space=pltpu.VMEM)


def place(row, col):
    return {"x": row // 2, "core": row % 2, "z": col // 4, "y": col % 4}


def index(at):
    return (at["x"] * 2 + at["core"]) * 16 + at["z"] * 4 + at["y"]


def pairs(phase, shift):
    moves = []
    for row in range(8):
        for col in range(16):
            at = place(row, col)
            to = dict(at)
            axis = ORDER[at["core"]][phase]
            to[axis] = (to[axis] + shift) % 4
            moves.append((index(at), index(to)))
    return moves


def send(value, phase, shift):
    return lax.ppermute(value, AXES, pairs(phase, shift))


def swap(value):
    return lax.ppermute(value, AXES, [(i, i ^ 16) for i in range(128)])


def route_kernel(tokens, scores, block):
    width, experts = tokens.shape[1], scores.shape[1]
    probs = jnp.exp(scores[...] - jnp.max(scores[...], axis=1, keepdims=True))
    probs = probs / jnp.sum(probs, axis=1, keepdims=True)
    block[:, :width] = tokens[...]
    block[:, width:] = jnp.zeros((block.shape[0], 128), block.dtype)
    block[:, width : width + experts] = probs.astype(block.dtype)


def join_kernel(places, *refs):
    out = refs[-1]
    for (row, col), ref in zip(places, refs[:-1]):
        out[row : row + ref.shape[0], col : col + ref.shape[1]] = ref[...]


def join(rows, cols, *pieces):
    arrays = [piece for piece, _, _ in pieces]
    places = tuple((row, col) for _, row, col in pieces)
    return pl.pallas_call(
        functools.partial(join_kernel, places),
        out_shape=jax.ShapeDtypeStruct((rows, cols), arrays[0].dtype),
        in_specs=[VMEM] * len(arrays),
        out_specs=VMEM,
        compiler_params=pltpu.CompilerParams(vmem_limit_bytes=6 << 20),
        name="join",
    )(*arrays)


def pack_kernel(gate, up, down, packed, kept, sems):
    per_group, _, units = gate.shape
    copies = [pltpu.make_async_copy(down, kept, sems.at[2 * per_group])]
    for j, weight in enumerate((gate, up)):
        for e in range(per_group):
            k = j * per_group + e
            to = packed.at[:, pl.ds(k * units, units)]
            copies.append(pltpu.make_async_copy(weight.at[e], to, sems.at[k]))
    for copy in copies:
        copy.start()
    for copy in copies:
        copy.wait()


def expert_kernel(piece_a, piece_b, spread, in_own, in_other, down_own, down_other, out_a, out_b, rows):
    half, width = out_a.shape
    rows[:half, :] = piece_a[...]
    rows[half:, :] = piece_b[...]
    weight = jnp.dot(rows[:, width:], spread[...], preferred_element_type=jnp.float32)
    hidden = []
    for k, w_in in enumerate((in_own, in_other)):
        both = jnp.dot(rows[:, :width], w_in[...], preferred_element_type=jnp.float32)
        units = both.shape[1] // 2
        gate = both[:, :units]
        value = gate / (1.0 + jnp.exp(-gate)) * both[:, units:] * weight[:, k * units : (k + 1) * units]
        hidden.append(value.astype(rows.dtype))
    step = width // 7
    for j in range(7):
        cols = slice(j * step, (j + 1) * step)
        part = jnp.dot(hidden[0], down_own[:, cols], preferred_element_type=jnp.float32)
        part = part + jnp.dot(hidden[1], down_other[:, cols], preferred_element_type=jnp.float32)
        part = part.astype(out_a.dtype)
        out_a[:, cols] = part[:half]
        out_b[:, cols] = part[half:]


def experts_of(piece_a, piece_b, weights):
    half, packed = piece_a.shape
    width = packed - 128
    kind = piece_a.dtype
    shape = jax.ShapeDtypeStruct((half, width), kind)
    return pl.pallas_call(
        expert_kernel,
        out_shape=(shape, shape),
        in_specs=[VMEM] * 7,
        out_specs=(VMEM,) * 2,
        scratch_shapes=[pltpu.VMEM((2 * half, packed), kind)],
        compiler_params=pltpu.CompilerParams(vmem_limit_bytes=12 << 20),
        cost_estimate=pl.CostEstimate(
            flops=4 * half * width * 1536, bytes_accessed=half * width * 8, transcendentals=half * 1024
        ),
        name="experts",
    )(piece_a, piece_b, *weights)


def pack(gate, up, down):
    per_group, width, units = gate.shape
    down = down.reshape(-1, width)
    return pl.pallas_call(
        pack_kernel,
        out_shape=(
            jax.ShapeDtypeStruct((width, 2 * per_group * units), gate.dtype),
            jax.ShapeDtypeStruct(down.shape, down.dtype),
        ),
        in_specs=[HBM] * 3,
        out_specs=(VMEM, VMEM),
        scratch_shapes=[pltpu.SemaphoreType.DMA((2 * per_group + 1,))],
        compiler_params=pltpu.CompilerParams(vmem_limit_bytes=2 << 20),
        name="pack",
    )(gate, up, down)


def add_kernel(starts, *refs):
    out = refs[-1]
    total = None
    for start, ref in zip(starts, refs[:-1]):
        piece = ref[start : start + out.shape[0], :].astype(jnp.float32)
        total = piece if total is None else total + piece
    out[...] = total.astype(out.dtype)


def add(rows, *pieces):
    arrays = [piece for piece, _ in pieces]
    starts = tuple(start for _, start in pieces)
    return pl.pallas_call(
        functools.partial(add_kernel, starts),
        out_shape=jax.ShapeDtypeStruct((rows, arrays[0].shape[1]), arrays[0].dtype),
        in_specs=[VMEM] * len(arrays),
        out_specs=VMEM,
        compiler_params=pltpu.CompilerParams(vmem_limit_bytes=6 << 20),
        name="add",
    )(*arrays)


def local(tokens, router_logits, expert_ids, w_gate, w_up, w_down):
    per_group, _, units = w_gate.shape
    count, width = tokens.shape
    packed = width + 128
    near = (1, 3, 2)
    experts = jnp.arange(router_logits.shape[1], dtype=jnp.int32)[None, :]
    chosen = expert_ids[:, 0:1] == experts
    for k in range(1, expert_ids.shape[1]):
        chosen = chosen | (expert_ids[:, k : k + 1] == experts)
    routing = jnp.where(chosen, router_logits, -jnp.inf)
    block = pl.pallas_call(
        route_kernel,
        out_shape=jax.ShapeDtypeStruct((count, packed), tokens.dtype),
        in_specs=[VMEM] * 2,
        out_specs=VMEM,
        compiler_params=pltpu.CompilerParams(vmem_limit_bytes=2 << 20),
        name="route",
    )(tokens, routing)
    got = [send(block, 0, -k) for k in near]
    gate_other, up_other, down_other = swap(w_gate), swap(w_up), swap(w_down)
    block = join(4 * count, packed, *((piece, k * count, 0) for k, piece in enumerate([block, *got])))
    row = lax.axis_index("row")
    spot = jnp.arange(2 * per_group * units)
    names = jnp.where(spot < per_group * units, row, row ^ 1) * per_group + spot // units % per_group
    spread = (jnp.arange(128)[:, None] == names[None, :]).astype(jnp.bfloat16)
    block, spread = lax.optimization_barrier((block, spread))

    got = [send(block, 1, -k) for k in near]
    in_own, down_own = pack(w_gate, w_up, w_down)
    in_other, down_other = pack(gate_other, up_other, down_other)
    weights = (spread, in_own, in_other, down_own, down_other)
    a0 = join(8 * count, packed, (block, 0, 0), (got[0], 4 * count, 0))
    b0 = join(8 * count, packed, (got[1], 0, 0), (got[2], 4 * count, 0))
    am, bp = send(a0, 2, 1), send(b0, 2, -1)
    oa, ob = send(am, 2, 1), send(bp, 2, -1)
    bm, ap = send(b0, 2, 1), send(a0, 2, -1)

    sa0, sb0 = experts_of(a0, b0, weights)
    sam, sbp = experts_of(am, bp, weights)
    soa, sob = experts_of(oa, ob, weights)
    sap, sbm = experts_of(ap, bm, weights)

    over_a = send(soa, 2, 1)
    over_b = send(sob, 2, -1)
    direct_b = send(sbp, 2, 1)
    direct_a = send(sam, 2, -1)
    part = 4 * count
    relay1 = send(add(part, (sap, part), (over_a, part)), 2, 1)
    relay2 = send(add(part, (sbm, part), (over_b, part)), 2, -1)
    relay0 = send(add(part, (sap, 0), (over_a, 0)), 2, 1)
    relay3 = send(add(part, (sbm, 0), (over_b, 0)), 2, -1)
    got = [send(add(part, (sa0, part), (direct_a, part), (relay1, 0)), 1, 1)]
    got.append(send(add(part, (sb0, part), (direct_b, part), (relay2, 0)), 1, 2))
    got.append(send(add(part, (sb0, 0), (direct_b, 0), (relay3, 0)), 1, 3))
    pieces = (add(part, (sa0, 0), (direct_a, 0), (relay0, 0)), *got)
    sums = [add(count, *((piece, k * count) for piece in pieces)) for k in range(4)]
    got = [send(sums[j], 0, k) for j, k in ((1, 1), (2, 3), (3, 2))]
    return add(count, *((piece, 0) for piece in (sums[0], *got)))


def solution(mesh):
    in_specs = (
        P(("row", "col"), None),
        P(("row", "col"), None),
        P(("row", "col"), None),
        P("row", None, "col"),
        P("row", None, "col"),
        P("row", "col", None),
    )
    out_specs = P(("row", "col"), None)
    return jax.shard_map(local, mesh=mesh, in_specs=in_specs, out_specs=out_specs, check_vma=False)
```

```python
import functools

import jax
import jax.numpy as jnp
from jax import lax
from jax.experimental import pallas as pl
from jax.experimental.pallas import tpu as pltpu
from jax.sharding import PartitionSpec as P


AXES = ("row", "col")
ORDER = (("y", "z", "x"), ("x", "y", "z"))
HBM = pl.BlockSpec(memory_space=pltpu.HBM)
VMEM = pl.BlockSpec(memory_space=pltpu.VMEM)


def place(row, col):
    return {"x": row // 2, "core": row % 2, "z": col // 4, "y": col % 4}


def index(at):
    return (at["x"] * 2 + at["core"]) * 16 + at["z"] * 4 + at["y"]


def pairs(phase, shift):
    moves = []
    for row in range(8):
        for col in range(16):
            at = place(row, col)
            to = dict(at)
            axis = ORDER[at["core"]][phase]
            to[axis] = to[axis] ^ shift
            moves.append((index(at), index(to)))
    return moves


def send(value, phase, shift):
    return lax.ppermute(value, AXES, pairs(phase, shift))


def swap(value):
    return lax.ppermute(value, AXES, [(i, i ^ 16) for i in range(128)])


def route_kernel(tokens, routing, block):
    width = tokens.shape[1]
    experts = 16
    logits = routing[:, :experts]
    names = lax.broadcasted_iota(jnp.int32, logits.shape, 1).astype(jnp.float32)
    chosen = routing[:, experts : experts + 1] == names
    for k in range(experts + 1, routing.shape[1]):
        chosen = chosen | (routing[:, k : k + 1] == names)
    scores = jnp.where(chosen, logits, -jnp.inf)
    scores = jnp.exp(scores - jnp.max(scores, axis=1, keepdims=True))
    probs = scores / jnp.sum(scores, axis=1, keepdims=True)
    block[:, :width] = tokens[...]
    block[:, width:] = jnp.zeros((block.shape[0], 128), block.dtype)
    block[:, width : width + experts] = probs.astype(block.dtype)


def join_kernel(places, *refs):
    out = refs[-1]
    for (row, col), ref in zip(places, refs[:-1]):
        out[row : row + ref.shape[0], col : col + ref.shape[1]] = ref[...]


def join(rows, cols, *pieces):
    arrays = [piece for piece, _, _ in pieces]
    places = tuple((row, col) for _, row, col in pieces)
    return pl.pallas_call(
        functools.partial(join_kernel, places),
        out_shape=jax.ShapeDtypeStruct((rows, cols), arrays[0].dtype),
        in_specs=[VMEM] * len(arrays),
        out_specs=VMEM,
        compiler_params=pltpu.CompilerParams(vmem_limit_bytes=6 << 20),
        name="join",
    )(*arrays)


def pack_kernel(gate, up, down, packed, kept, sems):
    per_group, _, units = gate.shape
    copies = [pltpu.make_async_copy(down, kept, sems.at[2 * per_group])]
    for j, weight in enumerate((gate, up)):
        for e in range(per_group):
            k = j * per_group + e
            to = packed.at[:, pl.ds(k * units, units)]
            copies.append(pltpu.make_async_copy(weight.at[e], to, sems.at[k]))
    for copy in copies:
        copy.start()
    for copy in copies:
        copy.wait()


def expert_kernel(piece_a, piece_b, spread, in_own, in_other, down_own, down_other, out_a, out_b, rows):
    half, width = out_a.shape
    rows[:half, :] = piece_a[...]
    rows[half:, :] = piece_b[...]
    weight = jnp.dot(rows[:, width:], spread[...], preferred_element_type=jnp.float32)
    hidden = []
    for k, w_in in enumerate((in_own, in_other)):
        both = jnp.dot(rows[:, :width], w_in[...], preferred_element_type=jnp.float32)
        units = both.shape[1] // 2
        gate = both[:, :units]
        value = gate / (1.0 + jnp.exp(-gate)) * both[:, units:] * weight[:, k * units : (k + 1) * units]
        hidden.append(value.astype(rows.dtype))
    step = width // 7
    for j in range(7):
        cols = slice(j * step, (j + 1) * step)
        part = jnp.dot(hidden[0], down_own[:, cols], preferred_element_type=jnp.float32)
        part = part + jnp.dot(hidden[1], down_other[:, cols], preferred_element_type=jnp.float32)
        part = part.astype(out_a.dtype)
        out_a[:, cols] = part[:half]
        out_b[:, cols] = part[half:]


def experts_of(piece_a, piece_b, weights):
    half, packed = piece_a.shape
    width = packed - 128
    kind = piece_a.dtype
    shape = jax.ShapeDtypeStruct((half, width), kind)
    return pl.pallas_call(
        expert_kernel,
        out_shape=(shape, shape),
        in_specs=[VMEM] * 7,
        out_specs=(VMEM,) * 2,
        scratch_shapes=[pltpu.VMEM((2 * half, packed), kind)],
        compiler_params=pltpu.CompilerParams(vmem_limit_bytes=12 << 20),
        cost_estimate=pl.CostEstimate(
            flops=4 * half * width * 1536, bytes_accessed=half * width * 8, transcendentals=half * 1024
        ),
        name="experts",
    )(piece_a, piece_b, *weights)


def pack(gate, up, down):
    per_group, width, units = gate.shape
    down = down.reshape(-1, width)
    return pl.pallas_call(
        pack_kernel,
        out_shape=(
            jax.ShapeDtypeStruct((width, 2 * per_group * units), gate.dtype),
            jax.ShapeDtypeStruct(down.shape, down.dtype),
        ),
        in_specs=[HBM] * 3,
        out_specs=(VMEM, VMEM),
        scratch_shapes=[pltpu.SemaphoreType.DMA((2 * per_group + 1,))],
        compiler_params=pltpu.CompilerParams(vmem_limit_bytes=2 << 20),
        name="pack",
    )(gate, up, down)


def add_kernel(starts, *refs):
    out = refs[-1]
    total = None
    for start, ref in zip(starts, refs[:-1]):
        piece = ref[start : start + out.shape[0], :].astype(jnp.float32)
        total = piece if total is None else total + piece
    out[...] = total.astype(out.dtype)


def add(rows, *pieces):
    arrays = [piece for piece, _ in pieces]
    starts = tuple(start for _, start in pieces)
    return pl.pallas_call(
        functools.partial(add_kernel, starts),
        out_shape=jax.ShapeDtypeStruct((rows, arrays[0].shape[1]), arrays[0].dtype),
        in_specs=[VMEM] * len(arrays),
        out_specs=VMEM,
        compiler_params=pltpu.CompilerParams(vmem_limit_bytes=6 << 20),
        name="add",
    )(*arrays)


def local(tokens, router_logits, expert_ids, w_gate, w_up, w_down):
    per_group, _, units = w_gate.shape
    count, width = tokens.shape
    packed = width + 128
    near = (1, 3, 2)
    routing = jnp.concatenate([router_logits, expert_ids.astype(jnp.float32)], axis=1)
    block = pl.pallas_call(
        route_kernel,
        out_shape=jax.ShapeDtypeStruct((count, packed), tokens.dtype),
        in_specs=[VMEM] * 2,
        out_specs=VMEM,
        compiler_params=pltpu.CompilerParams(vmem_limit_bytes=2 << 20),
        name="route",
    )(tokens, routing)
    got = [send(block, 0, k) for k in near]
    gate_other, up_other, down_other = swap(w_gate), swap(w_up), swap(w_down)
    block = join(4 * count, packed, *((piece, k * count, 0) for k, piece in enumerate([block, *got])))
    row = lax.axis_index("row")
    spot = jnp.arange(2 * per_group * units)
    names = jnp.where(spot < per_group * units, row, row ^ 1) * per_group + spot // units % per_group
    spread = (jnp.arange(128)[:, None] == names[None, :]).astype(jnp.bfloat16)
    block, spread = lax.optimization_barrier((block, spread))

    got = [send(block, 1, k) for k in near]
    in_own, down_own = pack(w_gate, w_up, w_down)
    in_other, down_other = pack(gate_other, up_other, down_other)
    weights = (spread, in_own, in_other, down_own, down_other)
    a0 = join(8 * count, packed, (block, 0, 0), (got[0], 4 * count, 0))
    b0 = join(8 * count, packed, (got[1], 0, 0), (got[2], 4 * count, 0))
    am, bp = send(a0, 2, 1), send(b0, 2, 3)
    oa, ob = send(am, 2, 3), send(bp, 2, 1)
    bm, ap = send(b0, 2, 1), send(a0, 2, 3)

    sa0, sb0 = experts_of(a0, b0, weights)
    sam, sbp = experts_of(am, bp, weights)
    soa, sob = experts_of(oa, ob, weights)
    sap, sbm = experts_of(ap, bm, weights)

    over_a = send(soa, 2, 3)
    over_b = send(sob, 2, 1)
    direct_b = send(sbm, 2, 1)
    direct_a = send(sap, 2, 3)

    part = 4 * count
    relay1 = send(add(part, (sam, part), (over_a, part)), 2, 1)
    relay2 = send(add(part, (sbp, part), (over_b, part)), 2, 3)
    relay0 = send(add(part, (sam, 0), (over_a, 0)), 2, 1)
    relay3 = send(add(part, (sbp, 0), (over_b, 0)), 2, 3)
    got = [send(add(part, (sa0, part), (direct_a, part), (relay1, 0)), 1, 1)]
    got.append(send(add(part, (sb0, part), (direct_b, part), (relay2, 0)), 1, 2))
    got.append(send(add(part, (sb0, 0), (direct_b, 0), (relay3, 0)), 1, 3))
    pieces = (add(part, (sa0, 0), (direct_a, 0), (relay0, 0)), *got)
    sums = [add(count, *((piece, k * count) for piece in pieces)) for k in range(4)]
    got = [send(sums[j], 0, k) for j, k in ((1, 1), (2, 3), (3, 2))]
    return add(count, *((piece, 0) for piece in (sums[0], *got)))


def solution(mesh):
    in_specs = (
        P(("row", "col"), None),
        P(("row", "col"), None),
        P(("row", "col"), None),
        P("row", None, "col"),
        P("row", None, "col"),
        P("row", "col", None),
    )
    out_specs = P(("row", "col"), None)
    return jax.shard_map(local, mesh=mesh, in_specs=in_specs, out_specs=out_specs, check_vma=False)
```

```python
import functools

import jax
import jax.numpy as jnp
from jax import lax
from jax.experimental import pallas as pl
from jax.experimental.pallas import tpu as pltpu
from jax.sharding import PartitionSpec as P


AXES = ("row", "col")
ORDER = (("y", "z", "x"), ("x", "y", "z"))
HBM = pl.BlockSpec(memory_space=pltpu.HBM)
VMEM = pl.BlockSpec(memory_space=pltpu.VMEM)


def place(row, col):
    return {"x": row // 2, "core": row % 2, "z": col // 4, "y": col % 4}


def index(at):
    return (at["x"] * 2 + at["core"]) * 16 + at["z"] * 4 + at["y"]


def pairs(phase, shift):
    moves = []
    for row in range(8):
        for col in range(16):
            at = place(row, col)
            to = dict(at)
            axis = ORDER[at["core"]][phase]
            to[axis] = to[axis] ^ shift
            moves.append((index(at), index(to)))
    return moves


def send(value, phase, shift):
    return lax.ppermute(value, AXES, pairs(phase, shift))


def swap(value):
    return lax.ppermute(value, AXES, [(i, i ^ 16) for i in range(128)])


def route_kernel(tokens, routing, block):
    width = tokens.shape[1]
    experts = 16
    logits = routing[:, :experts]
    names = lax.broadcasted_iota(jnp.int32, logits.shape, 1).astype(jnp.float32)
    chosen = routing[:, experts : experts + 1] == names
    for k in range(experts + 1, routing.shape[1]):
        chosen = chosen | (routing[:, k : k + 1] == names)
    scores = jnp.where(chosen, logits, -jnp.inf)
    scores = jnp.exp(scores - jnp.max(scores, axis=1, keepdims=True))
    probs = scores / jnp.sum(scores, axis=1, keepdims=True)
    block[:, :width] = tokens[...]
    block[:, width:] = jnp.zeros((block.shape[0], 128), block.dtype)
    block[:, width : width + experts] = probs.astype(block.dtype)


def join_kernel(places, *refs):
    out = refs[-1]
    for (row, col), ref in zip(places, refs[:-1]):
        out[row : row + ref.shape[0], col : col + ref.shape[1]] = ref[...]


def join(rows, cols, *pieces):
    arrays = [piece for piece, _, _ in pieces]
    places = tuple((row, col) for _, row, col in pieces)
    return pl.pallas_call(
        functools.partial(join_kernel, places),
        out_shape=jax.ShapeDtypeStruct((rows, cols), arrays[0].dtype),
        in_specs=[VMEM] * len(arrays),
        out_specs=VMEM,
        compiler_params=pltpu.CompilerParams(vmem_limit_bytes=6 << 20),
        name="join",
    )(*arrays)


def pack_kernel(gate, up, down, packed, kept, sems):
    per_group, _, units = gate.shape
    copies = [pltpu.make_async_copy(down, kept, sems.at[2 * per_group])]
    for j, weight in enumerate((gate, up)):
        for e in range(per_group):
            k = j * per_group + e
            to = packed.at[:, pl.ds(k * units, units)]
            copies.append(pltpu.make_async_copy(weight.at[e], to, sems.at[k]))
    for copy in copies:
        copy.start()
    for copy in copies:
        copy.wait()


def expert_kernel(count, *refs):
    pieces, (spread, in_own, in_other, down_own, down_other) = refs[:count], refs[count : count + 5]
    outs, rows = refs[count + 5 : -1], refs[-1]
    half, width = outs[0].shape
    for k, piece in enumerate(pieces):
        rows[k * half : (k + 1) * half, :] = piece[...]
    weight = jnp.dot(rows[:, width:], spread[...], preferred_element_type=jnp.float32)
    hidden = []
    for k, w_in in enumerate((in_own, in_other)):
        both = jnp.dot(rows[:, :width], w_in[...], preferred_element_type=jnp.float32)
        units = both.shape[1] // 2
        gate = both[:, :units]
        value = gate / (1.0 + jnp.exp(-gate)) * both[:, units:] * weight[:, k * units : (k + 1) * units]
        hidden.append(value.astype(rows.dtype))
    step = width // 7
    for j in range(7):
        cols = slice(j * step, (j + 1) * step)
        part = jnp.dot(hidden[0], down_own[:, cols], preferred_element_type=jnp.float32)
        part = part + jnp.dot(hidden[1], down_other[:, cols], preferred_element_type=jnp.float32)
        part = part.astype(rows.dtype)
        for k, out in enumerate(outs):
            out[:, cols] = part[k * half : (k + 1) * half]


def experts_of(pieces, weights):
    count = len(pieces)
    half, packed = pieces[0].shape
    width = packed - 128
    kind = pieces[0].dtype
    shape = jax.ShapeDtypeStruct((half, width), kind)
    return pl.pallas_call(
        functools.partial(expert_kernel, count),
        out_shape=(shape,) * count,
        in_specs=[VMEM] * (count + 5),
        out_specs=(VMEM,) * count,
        scratch_shapes=[pltpu.VMEM((count * half, packed), kind)],
        compiler_params=pltpu.CompilerParams(vmem_limit_bytes=12 << 20),
        cost_estimate=pl.CostEstimate(
            flops=4 * half * width * 1536, bytes_accessed=half * width * 8, transcendentals=half * 1024
        ),
        name="experts",
    )(*pieces, *weights)


def pack(gate, up, down):
    per_group, width, units = gate.shape
    down = down.reshape(-1, width)
    return pl.pallas_call(
        pack_kernel,
        out_shape=(
            jax.ShapeDtypeStruct((width, 2 * per_group * units), gate.dtype),
            jax.ShapeDtypeStruct(down.shape, down.dtype),
        ),
        in_specs=[HBM] * 3,
        out_specs=(VMEM, VMEM),
        scratch_shapes=[pltpu.SemaphoreType.DMA((2 * per_group + 1,))],
        compiler_params=pltpu.CompilerParams(vmem_limit_bytes=2 << 20),
        name="pack",
    )(gate, up, down)


def add_kernel(starts, *refs):
    out = refs[-1]
    total = None
    for start, ref in zip(starts, refs[:-1]):
        piece = ref[start : start + out.shape[0], :].astype(jnp.float32)
        total = piece if total is None else total + piece
    out[...] = total.astype(out.dtype)


def add(rows, *pieces):
    arrays = [piece for piece, _ in pieces]
    starts = tuple(start for _, start in pieces)
    return pl.pallas_call(
        functools.partial(add_kernel, starts),
        out_shape=jax.ShapeDtypeStruct((rows, arrays[0].shape[1]), arrays[0].dtype),
        in_specs=[VMEM] * len(arrays),
        out_specs=VMEM,
        compiler_params=pltpu.CompilerParams(vmem_limit_bytes=6 << 20),
        name="add",
    )(*arrays)


def local(tokens, router_logits, expert_ids, w_gate, w_up, w_down):
    per_group, _, units = w_gate.shape
    count, width = tokens.shape
    packed = width + 128
    near = (1, 3, 2)
    routing = jnp.concatenate([router_logits, expert_ids.astype(jnp.float32)], axis=1)
    block = pl.pallas_call(
        route_kernel,
        out_shape=jax.ShapeDtypeStruct((count, packed), tokens.dtype),
        in_specs=[VMEM] * 2,
        out_specs=VMEM,
        compiler_params=pltpu.CompilerParams(vmem_limit_bytes=2 << 20),
        name="route",
    )(tokens, routing)
    got = [send(block, 0, k) for k in near]
    gate_other, up_other, down_other = swap(w_gate), swap(w_up), swap(w_down)
    block = join(4 * count, packed, *((piece, k * count, 0) for k, piece in enumerate([block, *got])))
    row = lax.axis_index("row")
    spot = jnp.arange(2 * per_group * units)
    names = jnp.where(spot < per_group * units, row, row ^ 1) * per_group + spot // units % per_group
    spread = (jnp.arange(128)[:, None] == names[None, :]).astype(jnp.bfloat16)
    block, spread = lax.optimization_barrier((block, spread))

    got = [send(block, 1, k) for k in near]
    in_own, down_own = pack(w_gate, w_up, w_down)
    in_other, down_other = pack(gate_other, up_other, down_other)
    weights = (spread, in_own, in_other, down_own, down_other)
    a0 = join(8 * count, packed, (block, 0, 0), (got[0], 4 * count, 0))
    b0 = join(8 * count, packed, (got[1], 0, 0), (got[2], 4 * count, 0))
    am, bp = send(a0, 2, 1), send(b0, 2, 3)
    oa, ob = send(am, 2, 3), send(bp, 2, 1)
    bm, ap = send(b0, 2, 1), send(a0, 2, 3)

    sa0, sb0 = experts_of((a0, b0), weights)
    sam, sbp = experts_of((am, bp), weights)
    (soa,) = experts_of((oa,), weights)
    (sob,) = experts_of((ob,), weights)
    sap, sbm = experts_of((ap, bm), weights)

    over_a = send(soa, 2, 3)
    over_b = send(sob, 2, 1)
    direct_b = send(sbm, 2, 1)
    direct_a = send(sap, 2, 3)

    part = 4 * count
    relay1 = send(add(part, (sam, part), (over_a, part)), 2, 1)
    relay2 = send(add(part, (sbp, part), (over_b, part)), 2, 3)
    relay0 = send(add(part, (sam, 0), (over_a, 0)), 2, 1)
    relay3 = send(add(part, (sbp, 0), (over_b, 0)), 2, 3)
    got = [send(add(part, (sa0, part), (direct_a, part), (relay1, 0)), 1, 1)]
    got.append(send(add(part, (sb0, part), (direct_b, part), (relay2, 0)), 1, 2))
    got.append(send(add(part, (sb0, 0), (direct_b, 0), (relay3, 0)), 1, 3))
    pieces = (add(part, (sa0, 0), (direct_a, 0), (relay0, 0)), *got)
    sums = [add(count, *((piece, k * count) for piece in pieces)) for k in range(4)]
    got = [send(sums[j], 0, k) for j, k in ((1, 1), (2, 3), (3, 2))]
    return add(count, *((piece, 0) for piece in (sums[0], *got)))


def solution(mesh):
    in_specs = (
        P(("row", "col"), None),
        P(("row", "col"), None),
        P(("row", "col"), None),
        P("row", None, "col"),
        P("row", None, "col"),
        P("row", "col", None),
    )
    out_specs = P(("row", "col"), None)
    return jax.shard_map(local, mesh=mesh, in_specs=in_specs, out_specs=out_specs, check_vma=False)
```
